32 devices in a mesh: member: 2 (over x), graph: 8 (over z, y), chan: 2 (over core).
Axes of the slice: x: 2, y: 2, z: 4, core: 2. Of those that a mesh axis runs over, the one named last changes fastest.
Arguments:
- grid_state: bfloat16 [16384, 256], P(('member', 'graph')), parts along dimension 0, may hold values from -6 to 6
- w_src: bfloat16 [256, 512], P(None, 'chan'), may hold values from -0.375 to 0.375
- bias_src: float32 [512], P('chan'), may hold values from -3 to 3
- mesh_embed: bfloat16 [5120, 512], P('graph', 'chan'), may hold values from -6 to 6
- w_node: bfloat16 [512, 512], P('chan'), may hold values from -0.25 to 0.25
- w_dec: bfloat16 [512, 256], P('chan'), may hold values from -0.125 to 0.125
- slot_src: int32 [8, 8, 1024], P('graph'), may hold values from 0 to 1023, as said below
- slot_dst: int32 [8, 8, 1024], P(None, 'graph'), may hold values from 0 to 639, as said below
- slot_count: int32 [8, 8], replicated, may hold values from 1 to 1024, as said below
Outputs:
- grid_out: bfloat16 [16384, 256], P(('member', 'graph'), 'chan'), parts along dimension 0
The draws below stay inside these ranges and needn't reach their ends.
There are 2 independent parts, one for each index of `member`. The reference program is written for one: setup_inputs(seed, part) draws one part's arguments, and reference() takes and returns one part's arrays. A program takes and returns all parts, laid end to end along the dimension named above; an argument that names none is the same for every part. Nothing has to cross between parts.
Inputs may be any that keep to these rules, and one draw needn't show every extreme that they name: `slot_src`: slots at or past the live count hold arbitrary values in the same range. `slot_dst`: slots at or past the live count hold arbitrary values in the same range. slot_count[s, d] counts the live leading slots of the 1024 from shard s to shard d; in every draw some receiving shard has all 1024 slots live from every sender.
All inputs are finite; a program needn't handle non-finite values.
Results may differ from the reference program's by a relative error of at most 0.0056.
Values may be sent and summed in bfloat16 or wider, within the bound.
No kernel may reach another device: no remote copies, remote signals or barrier semaphores. Data moves between devices by JAX's collectives and lax.ppermute only.
A program may use at most 64 MiB of HBM per device.

```python
import jax
import jax.numpy as jnp
from jax import lax

C = 256
H = 512
GD = 1024
MD = 640
CAP = 1024
G = 8192
M = 5120
N_GRAPH = 8


def edge_tables(key):
    owners = jnp.arange(N_GRAPH, dtype=jnp.int32)
    offset = jnp.abs(owners[:, None] - owners[None, :])
    cycle_gap = jnp.minimum(offset, N_GRAPH - offset)
    near_bits = jax.random.randint(jax.random.fold_in(key, 12), (N_GRAPH, N_GRAPH), 0, 1 << 20)
    near_count = CAP // 2 + near_bits % (CAP - CAP // 2 + 1)
    levels = jax.random.randint(jax.random.fold_in(key, 11), (N_GRAPH,), 1, 5)
    tail_top = jnp.maximum(levels * (CAP // 16), 1)
    tail_bits = jax.random.randint(jax.random.fold_in(key, 14), (N_GRAPH, N_GRAPH), 0, 1 << 20)
    tail_pick = jax.random.randint(jax.random.fold_in(key, 15), (N_GRAPH, N_GRAPH), 0, 8)
    tail_count = jnp.where(tail_pick == 0, 1 + tail_bits % tail_top[None, :], 1)
    counts = jnp.where(cycle_gap <= 2, near_count, tail_count)
    fullest = jax.random.randint(jax.random.fold_in(key, 13), (), 0, N_GRAPH)
    return jnp.where(owners[None, :] == fullest, CAP, counts).astype(jnp.int32)


def draw_slot_count(key, part):
    return edge_tables(key)


def draw_slot_src(key, part):
    return jax.random.randint(jax.random.fold_in(key, 21), (N_GRAPH, N_GRAPH, CAP), 0, GD).astype(jnp.int32)


def draw_slot_dst(key, part):
    return jax.random.randint(jax.random.fold_in(key, 31), (N_GRAPH, N_GRAPH, CAP), 0, MD).astype(jnp.int32)


def block_scale(own_key, shape, shards, low, high):
    gain = 1.0
    for axis_at, blocks in shards:
        steps = jax.random.uniform(jax.random.fold_in(jax.random.fold_in(own_key, 6), axis_at), (blocks,), jnp.float32, low / len(shards), high / len(shards))
        gain = gain * jnp.repeat(jnp.exp(steps), shape[axis_at] // blocks).reshape((-1,) + (1,) * (len(shape) - 1 - axis_at))
    return gain


def scatter_about(rng, extent, spread, reach, cuts=(), kind=jnp.bfloat16):
    gain = block_scale(rng, extent, cuts, -0.22, 0.18) if cuts else 1.0
    array = jax.random.normal(rng, extent, jnp.float32) * spread * gain
    return jnp.minimum(jnp.maximum(array, -reach), reach).astype(kind)


def setup_inputs(seed: int = 0, part: int = 0) -> dict:
    arg_keys = jax.random.split(jax.random.key(seed), 10)
    own_keys = jax.random.split(jax.random.fold_in(arg_keys[9], part), 10)
    grid_state = scatter_about(own_keys[0], (G, C), 1.0, 6.0, ((0, 8),))
    w_src = scatter_about(arg_keys[1], (C, H), C ** -0.5, 0.375, ((1, 2),))
    bias_src = scatter_about(arg_keys[2], (H,), 0.5, 3.0, ((0, 2),), jnp.float32)
    mesh_embed = scatter_about(arg_keys[3], (M, H), 1.0, 6.0, ((0, 8), (1, 2)))
    w_node = scatter_about(arg_keys[4], (H, H), H ** -0.5, 0.25, ((0, 2),))
    w_dec = scatter_about(arg_keys[5], (H, C), (4 * H) ** -0.5, 0.125, ((0, 2),))
    slot_src = draw_slot_src(jax.random.fold_in(arg_keys[9], 71), part)
    slot_dst = draw_slot_dst(jax.random.fold_in(arg_keys[9], 71), part)
    slot_count = draw_slot_count(jax.random.fold_in(arg_keys[9], 71), part)
    return {"grid_state": grid_state, "w_src": w_src, "bias_src": bias_src, "mesh_embed": mesh_embed, "w_node": w_node, "w_dec": w_dec, "slot_src": slot_src, "slot_dst": slot_dst, "slot_count": slot_count}


def reference(grid_state, w_src, bias_src, mesh_embed, w_node, w_dec, slot_src, slot_dst, slot_count):
    positions = jnp.arange(CAP, dtype=jnp.int32)
    owners = jnp.arange(N_GRAPH, dtype=jnp.int32)

    def send_part(aggregate, sender):
        picked = jnp.take(grid_state, (sender * GD + slot_src[sender]).reshape(-1), axis=0)
        messages = jax.nn.silu(jnp.dot(picked, w_src, preferred_element_type=jnp.float32) + bias_src).astype(jnp.bfloat16)
        usable = (positions[None, :] < slot_count[sender][:, None]).reshape(-1)
        mesh_ids = (owners[:, None] * MD + slot_dst[sender]).reshape(-1).astype(jnp.int32)
        terms = jnp.where(usable[:, None], messages.astype(jnp.float32), jnp.zeros((), jnp.float32))
        return aggregate + jax.ops.segment_sum(terms, mesh_ids, num_segments=N_GRAPH * MD), None

    aggregate, unused = lax.scan(send_part, jnp.zeros((N_GRAPH * MD, H), jnp.float32), owners)
    hidden_pre = jnp.dot(aggregate.astype(jnp.bfloat16), w_node, preferred_element_type=jnp.float32)
    latent = (mesh_embed.astype(jnp.float32) + jax.nn.silu(hidden_pre)).astype(jnp.bfloat16)
    projected = jnp.dot(latent, w_dec, preferred_element_type=jnp.float32).astype(jnp.bfloat16)

    def decode_part(sender):
        usable = (positions[None, :] < slot_count[sender][:, None]).reshape(-1)
        mesh_ids = (owners[:, None] * MD + slot_dst[sender]).reshape(-1).astype(jnp.int32)
        returned = jnp.where(usable[:, None], jnp.take(projected, mesh_ids, axis=0).astype(jnp.float32), jnp.zeros((), jnp.float32))
        decoded = jax.ops.segment_sum(returned, slot_src[sender].reshape(-1).astype(jnp.int32), num_segments=GD)
        own_rows = lax.dynamic_slice_in_dim(grid_state, (sender * GD).astype(jnp.int32), GD, 0)
        return (own_rows.astype(jnp.float32) + decoded).astype(jnp.bfloat16)

    return lax.map(decode_part, owners).reshape(N_GRAPH * GD, C)
```

```python
import jax
import jax.numpy as jnp
from jax import lax
from jax.sharding import PartitionSpec as P

BF = jnp.bfloat16
F32 = jnp.float32


def swap_cores(x):
    return lax.ppermute(x, "chan", [(0, 1), (1, 0)])


def in_core_order(own, other, core, axis):
    return jnp.where(
        core == 0,
        jnp.concatenate([own, other], axis=axis),
        jnp.concatenate([other, own], axis=axis),
    )


def exchange_tables(tables, own_index, peers):
    bits = peers.bit_length() - 1
    if peers != 1 << bits:
        return lax.all_to_all(tables, "graph", 0, 0, tiled=True)
    tail = tables.shape[1:]
    x = tables
    for b in range(bits):
        step = 1 << b
        pairs = [(i, i ^ step) for i in range(peers)]
        x = x.reshape((peers // (2 * step), 2, step) + tail)
        upper = ((own_index // step) % 2) == 1
        kept = jnp.where(upper, x[:, 1], x[:, 0])
        given = jnp.where(upper, x[:, 0], x[:, 1])
        got = lax.ppermute(given, "graph", pairs)
        x = jnp.where(
            upper, jnp.stack([got, kept], axis=1), jnp.stack([kept, got], axis=1)
        ).reshape((peers,) + tail)
    return x


def gather_blocks(x, own_index, peers):
    pair = 2
    ring = peers // pair
    if ring != 4:
        return None
    z, y = own_index // pair, own_index % pair

    def index(dz, dy):
        return ((z + dz) % ring) * pair + (y + dy) % pair

    def from_z(v, dz):
        moves = [
            (((a + dz) % ring) * pair + b, a * pair + b) for a in range(ring) for b in range(pair)
        ]
        return lax.ppermute(v, "graph", moves)

    def from_y(v):
        return lax.ppermute(v, "graph", [(i, i ^ 1) for i in range(peers)])

    below = from_z(x, -1)
    above = from_z(x, 1)
    side = from_y(x)
    far = from_z(below, -1)
    side_above = from_z(side, 1)
    side_below = from_y(below)
    side_far = from_y(far)
    return [
        (x, own_index),
        (below, index(-1, 0)),
        (above, index(1, 0)),
        (side, index(0, 1)),
        (far, index(2, 0)),
        (side_above, index(1, 1)),
        (side_below, index(-1, 1)),
        (side_far, index(2, 1)),
    ]


def one_hot(ids, count, axis):
    if axis == 0:
        return (jnp.arange(count, dtype=jnp.int32)[:, None] == ids[None, :]).astype(BF)
    return (ids[:, None] == jnp.arange(count, dtype=jnp.int32)[None, :]).astype(BF)


def count_matrix(row_ids, row_count, col_ids, col_count):
    return jnp.dot(
        one_hot(row_ids, row_count, 0),
        one_hot(col_ids, col_count, 1),
        preferred_element_type=F32,
    ).astype(BF)


def on_device(
    grid_state, w_src, bias_src, mesh_embed, w_node, w_dec, slot_src, slot_dst, slot_count
):
    peers = lax.axis_size("graph")
    own = lax.axis_index("graph")
    core = lax.axis_index("chan")
    capacity = slot_src.shape[2]
    positions = jnp.arange(capacity, dtype=jnp.int32)
    grid_rows, channels = grid_state.shape
    mesh_rows = mesh_embed.shape[0]
    half_grid = grid_rows // 2
    half_mesh = mesh_rows // 2
    half_chan = channels // 2

    own_rows = lax.dynamic_slice_in_dim(grid_state, core * half_grid, half_grid, 0)
    blocks = gather_blocks(own_rows, own, peers)

    tables = exchange_tables(jnp.stack([slot_src[0], slot_dst[:, 0, :]], axis=1), own, peers)

    half_hidden = w_src.shape[1]
    other_embed = lax.dynamic_slice_in_dim(mesh_embed, (1 - core) * half_mesh, half_mesh, 0)
    own_embed = lax.dynamic_slice_in_dim(mesh_embed, core * half_mesh, half_mesh, 0)
    bias_other = swap_cores(bias_src[None, :])
    w_src_full = in_core_order(w_src, swap_cores(w_src), core, 1)
    w_node_full = in_core_order(w_node, swap_cores(w_node), core, 0)
    w_dec_full = in_core_order(w_dec, swap_cores(w_dec), core, 0)
    embed = in_core_order(own_embed, swap_cores(other_embed), core, 1)
    bias_full = in_core_order(bias_src[None, :], bias_other, core, 1)

    sent_counts = lax.dynamic_slice_in_dim(slot_count, own, 1, 0)[0]
    recv_counts = lax.dynamic_slice_in_dim(slot_count, own, 1, 1)[:, 0]
    in_src = tables[:, 0] - core * half_grid
    in_dst = jnp.where(positions[None, :] < recv_counts[:, None], slot_dst[:, 0, :], -1)
    out_src = jnp.where(positions[None, :] < sent_counts[:, None], slot_src[0], -1)
    out_dst = tables[:, 1] - core * half_mesh

    def row_of(table, p):
        return lax.dynamic_slice_in_dim(table, p, 1, 0)[0]

    def encode(block, p):
        pre = jnp.dot(block, w_src_full, preferred_element_type=F32) + bias_full
        messages = jax.nn.silu(pre).astype(BF)
        counts = count_matrix(row_of(in_dst, p), mesh_rows, row_of(in_src, p), half_grid)
        return jnp.dot(counts, messages, preferred_element_type=F32)

    def decode(block, p):
        counts = count_matrix(row_of(out_src, p), grid_rows, row_of(out_dst, p), half_mesh)
        return jnp.dot(counts, block, preferred_element_type=F32)

    def over_peers(block, found, apply, shape):
        if found is not None:
            total = None
            for piece, p in found:
                term = apply(piece, p)
                total = term if total is None else total + term
            return total
        everything = lax.all_gather(block, "graph")

        def step(total, item):
            piece, p = item
            return total + apply(piece, p), None

        return lax.scan(
            step, jnp.zeros(shape, F32), (everything, jnp.arange(peers, dtype=jnp.int32))
        )[0]

    partial = over_peers(own_rows, blocks, encode, (mesh_rows, 2 * half_hidden))
    kept = lax.dynamic_slice_in_dim(partial, core * half_mesh, half_mesh, 0)
    given = lax.dynamic_slice_in_dim(partial, (1 - core) * half_mesh, half_mesh, 0).astype(BF)
    aggregate = kept + swap_cores(given).astype(F32)
    hidden = jnp.dot(aggregate.astype(BF), w_node_full, preferred_element_type=F32)
    latent = (embed.astype(F32) + jax.nn.silu(hidden)).astype(BF)
    projected = jnp.dot(latent, w_dec_full, preferred_element_type=F32).astype(BF)

    returned = gather_blocks(projected, own, peers)
    decoded = over_peers(projected, returned, decode, (grid_rows, channels))
    kept = lax.dynamic_slice_in_dim(decoded, core * half_chan, half_chan, 1)
    given = lax.dynamic_slice_in_dim(decoded, (1 - core) * half_chan, half_chan, 1).astype(BF)
    own_cols = lax.dynamic_slice_in_dim(grid_state, core * half_chan, half_chan, 1)
    return (own_cols.astype(F32) + kept + swap_cores(given).astype(F32)).astype(BF)


def solution(mesh):
    placed = (
        P(("member", "graph"), None),
        P(None, "chan"),
        P("chan"),
        P("graph", "chan"),
        P("chan", None),
        P("chan", None),
        P("graph", None, None),
        P(None, "graph", None),
        P(),
    )
    return jax.shard_map(
        on_device,
        mesh=mesh,
        in_specs=placed,
        out_specs=P(("member", "graph"), "chan"),
        check_vma=False,
    )
```
